32 devices in a mesh: seq: 2 (over core), width: 4 (over y, x), dp: 4 (over z).
Axes of the slice: x: 2, y: 2, z: 4, core: 2. Of those that a mesh axis runs over, the one named last changes fastest.
Arguments:
- inputs: bfloat16 [4, 512, 5376], P('dp', 'seq', 'width'), may hold values from -6 to 6
- out_grad: bfloat16 [4, 512, 5376], P('dp', 'seq', 'width'), may hold values from -6 to 6
- gate_a: bfloat16 [16, 336, 336], P('width'), may hold values from -0.3125 to 0.3125
- gate_x: bfloat16 [16, 336, 336], P('width'), may hold values from -0.3125 to 0.3125
- bias_a: float32 [5376], P('width'), may hold values from -1.5 to 1.5
- bias_x: float32 [5376], P('width'), may hold values from -1.5 to 1.5
- decay_param: float32 [5376], P('width'), may hold values from -12 to -4.5
- segment_ids: int32 [4, 512], P('dp', 'seq'), may hold values from 0 to 3, never falling along the last dimension, each value on 1 to 256 neighbouring positions
Outputs:
- input_grad: bfloat16 [4, 512, 5376], P('dp', 'seq', 'width')
- gate_a_grad: float32 [16, 336, 336], P('width')
- gate_x_grad: float32 [16, 336, 336], P('width')
- bias_a_grad: float32 [5376], P('width')
- bias_x_grad: float32 [5376], P('width')
- decay_grad: float32 [5376], P('width')
The draws below stay inside these ranges and needn't reach their ends.
All inputs are finite; a program needn't handle non-finite values.
Results may differ from the reference program's by a relative error of at most 0.0029.
Values sent between devices are 32-bit elements; how exact they have to be, the bound alone decides.
No kernel may reach another device: no remote copies, remote signals or barrier semaphores. Data moves between devices by JAX's collectives and lax.ppermute only.
A program may use at most 128 MiB of HBM per device.

```python
import math
import jax
import jax.numpy as jnp
import numpy as np
from jax import lax

H = 16
K = 336
R = 5376
LENGTH = 512
BATCH = 4


def draw_decay_param(key, part):
    return jax.random.uniform(key, (R,), jnp.float32, -11.0, -4.5)


def block_levels(key, dims, shards, low, largest):
    level, own = 1.0, jax.random.fold_in(key, 6)
    for dim, shards_of in shards:
        steps = jnp.exp(jax.random.uniform(jax.random.fold_in(own, dim), (shards_of,), jnp.float32, low / len(shards), largest / len(shards)))
        level = level * jnp.repeat(steps, dims[dim] // shards_of).reshape([-1 if axis == dim else 1 for axis in range(len(dims))])
    return level


def length_profile(amount, total, bound, lean):
    weights = [(1 << 20) // math.isqrt(rank ** lean) + 1 for rank in range(2, amount + 1)]
    surplus, holding = total - bound - (amount - 1), [1] * (amount - 1)
    while surplus > 0:
        candidates = [i for i in range(amount - 1) if holding[i] < bound]
        whole, budget = sum([weights[i] for i in candidates]), surplus
        for i in candidates:
            more = min(bound - holding[i], max(1, budget * weights[i] // whole), surplus)
            holding[i] = holding[i] + more
            surplus = surplus - more
    return np.array([bound] + holding)


def uneven(stream_key, count, total, reach, lean):
    if count == 2:
        one = jax.random.randint(stream_key, (), max(1, total - reach), min(reach, total - 1) + 1)
        return jnp.stack([one, total - one])
    tallies = jnp.asarray(length_profile(count, total, reach, lean), jnp.int32)
    couples = (count - 1) // 2
    source_of, sink = tallies[1:1 + 2 * couples:2], tallies[2:2 + 2 * couples:2]
    room = jnp.minimum(source_of - 1, reach - sink)
    moved = jax.random.randint(jax.random.fold_in(stream_key, 1), (couples,), 0, 1 << 20) % (room + 1)
    tallies = tallies.at[1:1 + 2 * couples:2].set(source_of - moved).at[2:2 + 2 * couples:2].set(sink + moved)
    return tallies[jax.random.permutation(jax.random.fold_in(stream_key, 2), count)]


def normal_values(stream_key, extent, scale, reach, cuts=(), kind=jnp.bfloat16):
    loudness = block_levels(stream_key, extent, cuts, -0.22, 0.18) if cuts else 1.0
    drawn = jax.random.normal(stream_key, extent, jnp.float32) * scale * loudness
    return jnp.minimum(jnp.maximum(drawn, -reach), reach).astype(kind)


def setup_inputs(seed: int = 0) -> dict:
    key_list = jax.random.split(jax.random.key(seed), 9)
    inputs = normal_values(key_list[0], (BATCH, LENGTH, R), 1.0, 6.0, ((0, 4), (1, 2), (2, 4)))
    out_grad = normal_values(key_list[1], (BATCH, LENGTH, R), 1.0, 6.0, ((0, 4), (1, 2), (2, 4)))
    gate_a = normal_values(key_list[2], (H, K, K), K ** -0.5, 0.3125, ((0, 4),))
    gate_x = normal_values(key_list[3], (H, K, K), K ** -0.5, 0.3125, ((0, 4),))
    bias_a = jnp.clip(jax.random.uniform(key_list[4], (R,), jnp.float32, -1.5, 1.5) * block_levels(key_list[4], (R,), ((0, 4),), -0.4, 0.0), -1.5, 1.5)
    bias_x = jnp.clip(jax.random.uniform(key_list[5], (R,), jnp.float32, -1.5, 1.5) * block_levels(key_list[5], (R,), ((0, 4),), -0.4, 0.0), -1.5, 1.5)
    decay_param = draw_decay_param(jax.random.fold_in(key_list[8], 71), 0)
    segment_ids = jax.vmap(lambda own: jnp.searchsorted(jnp.cumsum(uneven(own, 4, LENGTH, LENGTH // 2, 1)), jnp.arange(LENGTH), side="right"))(jax.random.split(key_list[7], BATCH)).reshape((BATCH, LENGTH)).astype(jnp.int32)
    return dict(inputs=inputs, out_grad=out_grad, gate_a=gate_a, gate_x=gate_x, bias_a=bias_a, bias_x=bias_x, decay_param=decay_param, segment_ids=segment_ids)


def combine(earlier, later):
    return (earlier[0] * later[0], earlier[1] * later[0] + later[1])

def per_block(items):
    xb, dyb, wa, wx, ba, bx, lam, keep = items
    batch, length, width_k = xb.shape
    flat = xb.reshape(batch * length, width_k)
    pre_a = jnp.dot(flat, wa, preferred_element_type=jnp.float32).reshape(batch, length, width_k) + ba
    pre_x = jnp.dot(flat, wx, preferred_element_type=jnp.float32).reshape(batch, length, width_k) + bx
    rate = jax.nn.sigmoid(pre_a)
    ingate = jax.nn.sigmoid(pre_x)
    soft = jax.nn.softplus(lam)
    log_a = -8.0 * rate * soft
    decay = jnp.exp(log_a)
    abar = keep * decay
    mult = jnp.where(keep > 0.5, jnp.sqrt(-jnp.expm1(2.0 * log_a)), 1.0)
    xf = xb.astype(jnp.float32)
    dyf = dyb.astype(jnp.float32)
    drive = mult * ingate * xf

    def forward(state, pair):
        return (pair[0] * state + pair[1], state)
    start = jnp.zeros((batch, width_k), jnp.float32)
    last, h_prev = lax.scan(forward, start, (jnp.swapaxes(abar, 0, 1), jnp.swapaxes(drive, 0, 1)))
    h_prev = jnp.swapaxes(h_prev, 0, 1)
    dnext = jnp.concatenate([abar[:, 1:], jnp.zeros((batch, 1, width_k), jnp.float32)], 1)

    def backward(carry, pair):
        value = pair[1] + pair[0] * carry
        return (value, value)
    first, grad = lax.scan(backward, start, (jnp.swapaxes(dnext, 0, 1), jnp.swapaxes(dyf, 0, 1)), reverse=True)
    grad = jnp.swapaxes(grad, 0, 1)
    wsum = keep * (decay * grad * h_prev - grad * ingate * xf * decay * decay / mult)
    dpre_a = -8.0 * soft * rate * (1.0 - rate) * wsum
    dpre_x = grad * mult * xf * ingate * (1.0 - ingate)
    da_b = dpre_a.astype(jnp.bfloat16).reshape(batch * length, width_k)
    dx_b = dpre_x.astype(jnp.bfloat16).reshape(batch * length, width_k)
    back = jnp.dot(da_b, wa.T, preferred_element_type=jnp.float32) + jnp.dot(dx_b, wx.T, preferred_element_type=jnp.float32)
    input_grad = (grad * mult * ingate + back.reshape(batch, length, width_k)).astype(jnp.bfloat16)
    grad_a = jnp.dot(flat.T, da_b, preferred_element_type=jnp.float32)
    grad_x = jnp.dot(flat.T, dx_b, preferred_element_type=jnp.float32)
    bias_ga = lax.optimization_barrier(jnp.sum(dpre_a, (0, 1)))
    bias_gx = lax.optimization_barrier(jnp.sum(dpre_x, (0, 1)))
    decay_g = jax.nn.sigmoid(lam) * lax.optimization_barrier(jnp.sum(-8.0 * rate * wsum, (0, 1)))
    return (input_grad, grad_a, grad_x, bias_ga, bias_gx, decay_g)

def reference(inputs, out_grad, gate_a, gate_x, bias_a, bias_x, decay_param, segment_ids):
    batch, length, chans = inputs.shape
    blocks, width_k = (gate_a.shape[0], gate_a.shape[1])
    before = jnp.concatenate([segment_ids[:, :1], segment_ids[:, :-1]], 1)
    position = jnp.arange(length, dtype=jnp.int32)
    reset = (segment_ids != before) | (position[None, :] == 0)
    keep = jnp.where(reset, 0.0, 1.0).astype(jnp.float32)[:, :, None]
    xs = jnp.transpose(inputs.reshape(batch, length, blocks, width_k), (2, 0, 1, 3))
    dys = jnp.transpose(out_grad.reshape(batch, length, blocks, width_k), (2, 0, 1, 3))
    keeps = jnp.broadcast_to(keep[None], (blocks, batch, length, 1))
    outs = lax.map(per_block, (xs, dys, gate_a, gate_x, bias_a.reshape(blocks, width_k), bias_x.reshape(blocks, width_k), decay_param.reshape(blocks, width_k), keeps))
    input_grad = jnp.transpose(outs[0], (1, 2, 0, 3)).reshape(batch, length, chans)
    return (input_grad, outs[1], outs[2], outs[3].reshape(chans), outs[4].reshape(chans), outs[5].reshape(chans))
```

```python
import functools

import jax
import jax.numpy as jnp
from jax import lax
from jax.experimental import pallas as pl
from jax.experimental.pallas import tpu as pltpu
from jax.sharding import PartitionSpec as P

LANES = 128
ROWS = 8
F32 = jnp.float32
BF16 = jnp.bfloat16


def shifted(value, axis, steps):
    count = lax.axis_size(axis)
    initial, last = (max(0, -steps), min(count, count - steps))
    return lax.ppermute(value, axis, [(source, source + steps) for source in range(initial, last)])


def carried_in(value, axis, join, neutral, backward):
    count, mine = (lax.axis_size(axis), lax.axis_index(axis))
    pieces = jax.tree.map(lambda part: lax.all_gather(part, axis), value)
    if backward:
        pieces = jax.tree.map(lambda part: part[::-1], pieces)
        mine = count - 1 - mine
    running = jax.tree.map(
        lambda part, zero: jnp.full_like(part, 0) + jnp.asarray(zero, part.dtype), value, neutral
    )

    def hop(position, running):
        longer = join(running, jax.tree.map(lambda part: part[position], pieces))
        return jax.tree.map(lambda new, old: jnp.where(position < mine, new, old), longer, running)

    return lax.fori_loop(0, count - 1, hop, running)


def combine(earlier, later):
    return (earlier[0] * later[0], earlier[1] * later[0] + later[1])


def general(inputs, out_grad, gate_a, gate_x, bias_a, bias_x, decay_param, segment_ids):
    batch, count, chans = inputs.shape
    blocks, width_k = (gate_a.shape[0], gate_a.shape[1])
    span_len = 8
    groups = count // span_len
    blocked = inputs.reshape(batch, count, blocks, width_k)
    pre_a = (
        jnp.einsum("stbk,bkj->stbj", blocked, gate_a, preferred_element_type=jnp.float32).reshape(
            batch, count, chans
        )
        + bias_a
    )
    pre_x = (
        jnp.einsum("stbk,bkj->stbj", blocked, gate_x, preferred_element_type=jnp.float32).reshape(
            batch, count, chans
        )
        + bias_x
    )
    rate = jax.nn.sigmoid(pre_a)
    ingate = jax.nn.sigmoid(pre_x)
    soft = jax.nn.softplus(decay_param)
    log_a = -8.0 * rate * soft
    decay = jnp.exp(log_a)
    shifted_ids = segment_ids + 1
    before = shifted(shifted_ids[:, -1:], "seq", 1)
    previous = jnp.concatenate([before, shifted_ids[:, :-1]], 1)
    position = lax.axis_index("seq") * count + jnp.arange(count, dtype=jnp.int32)
    reset = (shifted_ids != previous) | (position[None, :] == 0)
    keep = jnp.where(reset, 0.0, 1.0).astype(jnp.float32)[:, :, None]
    abar = keep * decay
    mult = jnp.where(keep > 0.5, jnp.sqrt(-jnp.expm1(2.0 * log_a)), 1.0)
    xf = inputs.astype(jnp.float32)
    dyf = out_grad.astype(jnp.float32)
    drive = mult * ingate * xf
    cum_log = jnp.cumsum(log_a.reshape(batch, groups, span_len, chans), 2)
    cum_reset = jnp.cumsum(
        jnp.where(reset, 1.0, 0.0).astype(jnp.float32).reshape(batch, groups, span_len), 2
    )
    order = jnp.arange(span_len, dtype=jnp.int32)
    lower = order[:, None] >= order[None, :]
    linked = (cum_reset[:, :, :, None] == cum_reset[:, :, None, :]) & lower
    spread = cum_log[:, :, :, None, :] - cum_log[:, :, None, :, :]
    factor = jnp.where(linked[..., None], jnp.exp(jnp.minimum(spread, 0.0)), 0.0)
    state_loc = jnp.einsum(
        "bntsc,bnsc->bntc",
        factor,
        drive.reshape(batch, groups, span_len, chans),
        precision=lax.Precision.HIGHEST,
    )
    grad_loc = jnp.einsum(
        "bntsc,bntc->bnsc",
        factor,
        dyf.reshape(batch, groups, span_len, chans),
        precision=lax.Precision.HIGHEST,
    )
    from_start = jnp.exp(cum_log) * jnp.where(cum_reset == 0.0, 1.0, 0.0)[..., None]
    to_end = (
        jnp.exp(cum_log[:, :, -1:, :] - cum_log)
        * jnp.where(cum_reset == cum_reset[:, :, -1:], 1.0, 0.0)[..., None]
    )
    group_prod = from_start[:, :, -1]
    group_state = state_loc[:, :, -1]
    group_grad = abar.reshape(batch, groups, span_len, chans)[:, :, 0] * grad_loc[:, :, 0]
    fwd_p, fwd_s = lax.associative_scan(combine, (group_prod, group_state), axis=1)
    bwd_p, bwd_s = lax.associative_scan(combine, (group_prod, group_grad), reverse=True, axis=1)
    forward_sum = (fwd_p[:, -1], fwd_s[:, -1])
    backward_sum = (bwd_p[:, 0], bwd_s[:, 0])
    unit = jnp.ones((batch, chans), jnp.float32)
    naught = jnp.zeros((batch, chans), jnp.float32)
    state_in = carried_in(forward_sum, "seq", combine, (unit, naught), False)[1]
    grad_in = carried_in(backward_sum, "seq", combine, (unit, naught), True)[1]
    excl_p = jnp.concatenate([unit[:, None], fwd_p[:, :-1]], 1)
    excl_s = jnp.concatenate([naught[:, None], fwd_s[:, :-1]], 1)
    entering = excl_s + excl_p * state_in[:, None, :]
    later_p = jnp.concatenate([bwd_p[:, 1:], unit[:, None]], 1)
    later_s = jnp.concatenate([bwd_s[:, 1:], naught[:, None]], 1)
    leaving = later_s + later_p * grad_in[:, None, :]
    state = (state_loc + from_start * entering[:, :, None, :]).reshape(batch, count, chans)
    grad = (grad_loc + to_end * leaving[:, :, None, :]).reshape(batch, count, chans)
    wsum = grad * (state - drive) - keep * (grad * ingate * xf * decay * decay / mult)
    dpre_a = -8.0 * soft * rate * (1.0 - rate) * wsum
    dpre_x = grad * mult * xf * ingate * (1.0 - ingate)
    da_b = dpre_a.astype(jnp.bfloat16).reshape(batch, count, blocks, width_k)
    dx_b = dpre_x.astype(jnp.bfloat16).reshape(batch, count, blocks, width_k)
    back = jnp.einsum(
        "stbj,bkj->stbk", da_b, gate_a, preferred_element_type=jnp.float32
    ) + jnp.einsum("stbj,bkj->stbk", dx_b, gate_x, preferred_element_type=jnp.float32)
    input_grad = (grad * mult * ingate + back.reshape(batch, count, chans)).astype(jnp.bfloat16)
    local_a = jnp.einsum("stbk,stbj->bkj", blocked, da_b, preferred_element_type=jnp.float32)
    local_x = jnp.einsum("stbk,stbj->bkj", blocked, dx_b, preferred_element_type=jnp.float32)
    bias_ga = jnp.sum(dpre_a, (0, 1))
    bias_gx = jnp.sum(dpre_x, (0, 1))
    decay_g = jnp.sum(-8.0 * rate * wsum, (0, 1))
    grad_a, grad_x, bias_ga, bias_gx, decay_g = lax.psum(
        (local_a, local_x, bias_ga, bias_gx, decay_g), ("seq", "dp")
    )
    return (input_grad, grad_a, grad_x, bias_ga, bias_gx, jax.nn.sigmoid(decay_param) * decay_g)


def minus_expm1(value, exp_value):
    series = 1.0 + value * (1.0 / 8.0)
    for term in (7, 6, 5, 4, 3, 2):
        series = 1.0 + value * (1.0 / term) * series
    return jnp.where(value > -0.25, -value * series, 1.0 - exp_value)


def block_kernel(
    core_ref, own_x, own_dy, other, own_seg, wa_ref, wx_ref, ba_ref, bx_ref, soft_ref,
    ga_ref, gx_ref, ig_own, ig_other,
    x_s, seg_s, ab_s, u_s, dy_s, r_s, k2_s, k3_s, mi_s, da_s, dx_s,
):
    count, width = own_x.shape
    total = 2 * count
    core = core_ref[0]
    mine = pl.ds(pl.multiple_of(core * count, count), count)
    theirs = pl.ds(pl.multiple_of((1 - core) * count, count), count)
    x_s[mine, :] = own_x[...]
    x_s[theirs, :] = other[0, :, :width].astype(BF16)
    seg_s[pl.ds(pl.multiple_of(ROWS + core * count, ROWS), count), :] = own_seg[...]
    seg_s[pl.ds(pl.multiple_of(ROWS + (1 - core) * count, ROWS), count), :] = other[2, :, :LANES]
    seg_s[:ROWS, :] = jnp.zeros((ROWS, LANES), F32)

    wa = wa_ref[0]
    wx = wx_ref[0]
    ba = ba_ref[0]
    bx = bx_ref[0]
    soft = soft_ref[0]
    tiles = -(-width // LANES)
    piece = 128
    edges = [(t * LANES, min(width, (t + 1) * LANES)) for t in range(tiles)]

    def put(ref, rows, value):
        for tile, (low, high) in enumerate(edges):
            ref[tile, rows, : high - low] = value[:, low:high]

    def get(ref, rows):
        return jnp.concatenate([ref[tile, rows, :] for tile in range(tiles)], 1)[:, :width]

    put(dy_s, mine, own_dy[...].astype(F32))
    put(dy_s, theirs, other[1, :, :width])

    def gates(step, _):
        base = pl.multiple_of(step * piece, piece)
        rows = pl.ds(base, piece)
        xb = x_s[rows, :]
        xf = xb.astype(F32)
        rate = jax.nn.sigmoid(jnp.dot(xb, wa, preferred_element_type=F32) + ba)
        ingate = jax.nn.sigmoid(jnp.dot(xb, wx, preferred_element_type=F32) + bx)
        log_a = -8.0 * rate * soft
        decay = jnp.exp(log_a)
        seg = seg_s[pl.ds(pl.multiple_of(ROWS + base, ROWS), piece), :]
        seg_prev = seg_s[pl.ds(ROWS - 1 + base, piece), :]
        place = base + lax.broadcasted_iota(jnp.int32, (piece, LANES), 0)
        keep1 = jnp.where((seg != seg_prev) | (place == 0), 0.0, 1.0)
        keep = jnp.concatenate([keep1] * tiles, 1)[:, :width]
        two = 2.0 * log_a
        power = jnp.maximum(minus_expm1(two, decay * decay), 1e-37)
        inv = lax.rsqrt(power)
        mult = jnp.where(keep > 0.5, power * inv, 1.0)
        mi = mult * ingate
        put(ab_s, rows, keep * decay)
        put(u_s, rows, mi * xf)
        r_s[rows, :] = rate
        k2_s[rows, :] = ingate * xf * decay * inv
        k3_s[rows, :] = xf * (1.0 - ingate)
        mi_s[rows, :] = mi
        return 0

    lax.fori_loop(0, total // piece, gates, 0)

    steps = total // ROWS
    every = range(tiles)

    def at(step):
        return pl.ds(step, ROWS, stride=steps)

    zero = jnp.zeros((ROWS, LANES), F32)

    def ends(step, carry):
        late = steps - 1 - step
        out = []
        for tile, (state, prod, back) in zip(every, carry):
            decay = ab_s[tile, at(step), :]
            state = decay * state + u_s[tile, at(step), :]
            back = ab_s[tile, at(late), :] * (dy_s[tile, at(late), :] + back)
            out.append((state, decay * prod, back))
        return out

    found = lax.fori_loop(0, steps, ends, [(zero, zero + 1.0, zero)] * tiles, unroll=8)
    entering = []
    for state, prod, back in found:
        run = jnp.zeros((1, LANES), F32)
        firsts = []
        for row in range(ROWS):
            firsts.append(run)
            run = state[row : row + 1] + prod[row : row + 1] * run
        run = jnp.zeros((1, LANES), F32)
        lasts = []
        for row in reversed(range(ROWS)):
            lasts.append(run)
            run = back[row : row + 1] + prod[row : row + 1] * run
        entering.append((jnp.concatenate(firsts, 0), jnp.concatenate(lasts[::-1], 0)))

    def scan(step, carry):
        late = steps - 1 - step
        out = []
        for tile, (state, back) in zip(every, carry):
            drive = u_s[tile, at(step), :]
            u_s[tile, at(step), :] = state
            state = ab_s[tile, at(step), :] * state + drive
            grad = dy_s[tile, at(late), :] + back
            dy_s[tile, at(late), :] = grad
            out.append((state, ab_s[tile, at(late), :] * grad))
        return out

    lax.fori_loop(0, steps, scan, entering, unroll=8)
    zero = jnp.zeros((ROWS, width), F32)

    def gradients(step, sums):
        rows = pl.ds(pl.multiple_of(step * piece, piece), piece)
        grad = get(dy_s, rows)
        rate = r_s[rows, :]
        q = -8.0 * rate * get(ab_s, rows) * grad * (get(u_s, rows) - k2_s[rows, :])
        dpre_a = soft * (1.0 - rate) * q
        direct = grad * mi_s[rows, :]
        dpre_x = direct * k3_s[rows, :]
        put(dy_s, rows, direct)
        da_s[rows, :] = dpre_a.astype(BF16)
        dx_s[rows, :] = dpre_x.astype(BF16)
        shape = (piece // ROWS, ROWS, width)
        return tuple(
            acc + jnp.sum(v.reshape(shape), 0) for acc, v in zip(sums, (dpre_a, q, dpre_x))
        )

    sum_a, sum_q, sum_x = lax.fori_loop(0, total // piece, gradients, (zero, zero, zero))
    row_id = lax.broadcasted_iota(jnp.int32, (ROWS, width), 0)
    across = (((0,), (0,)), ((), ()))
    x_all = x_s[...]
    ga_ref[:width, :] = lax.dot_general(x_all, da_s[...], across, preferred_element_type=F32)
    gx_ref[:width, :] = lax.dot_general(x_all, dx_s[...], across, preferred_element_type=F32)
    tot_a = jnp.sum(sum_a, 0, keepdims=True)
    tot_q = jnp.sum(sum_q, 0, keepdims=True)
    tot_x = jnp.sum(sum_x, 0, keepdims=True)
    ga_ref[width:, :] = jnp.where(row_id == 0, tot_a, jnp.where(row_id == 1, tot_q, 0.0))
    gx_ref[width:, :] = jnp.where(row_id == 0, tot_x, 0.0)
    along = (((1,), (1,)), ((), ()))

    def returned(where):
        back = lax.dot_general(da_s[where, :], wa, along, preferred_element_type=F32)
        back += lax.dot_general(dx_s[where, :], wx, along, preferred_element_type=F32)
        return get(dy_s, where) + back

    ig_other[...] = returned(theirs)
    ig_own[...] = returned(mine)


def run_block(which, core, own_x, own_dy, other, own_seg, gate_a, gate_x, bias_a, bias_x, soft):
    count, width = own_x.shape
    blocks = gate_a.shape[0]
    per_core = blocks // 2
    total = 2 * count

    def whole(shape):
        return pl.BlockSpec(shape, lambda i, c: (0,) * len(shape))

    def picked(rows):
        return pl.BlockSpec((1, rows, width), lambda i, c: (per_core * c[0] + which, 0, 0))

    f32 = functools.partial(pltpu.VMEM, dtype=F32)
    wide = (total, width)
    tiled = (-(-width // LANES), total, LANES)
    return pl.pallas_call(
        block_kernel,
        grid_spec=pltpu.PrefetchScalarGridSpec(
            num_scalar_prefetch=1,
            grid=(1,),
            in_specs=[
                whole(own_x.shape), whole(own_dy.shape), whole(other.shape), whole(own_seg.shape),
                picked(width), picked(width), picked(1), picked(1), picked(1),
            ],
            out_specs=[
                whole((width + ROWS, width)), whole((width + ROWS, width)),
                whole((count, width)), whole((count, width)),
            ],
            scratch_shapes=[
                pltpu.VMEM(wide, BF16), f32((total + ROWS, LANES)), f32(tiled), f32(tiled), f32(tiled),
                f32(wide), f32(wide), f32(wide), f32(wide), pltpu.VMEM(wide, BF16), pltpu.VMEM(wide, BF16),
            ],
        ),
        out_shape=[
            jax.ShapeDtypeStruct((width + ROWS, width), F32),
            jax.ShapeDtypeStruct((width + ROWS, width), F32),
            jax.ShapeDtypeStruct((count, width), F32),
            jax.ShapeDtypeStruct((count, width), F32),
        ],
        cost_estimate=pl.CostEstimate(
            flops=12 * total * width * width, bytes_accessed=8 * total * width, transcendentals=6 * total * width
        ),
    )(core, own_x, own_dy, other, own_seg, gate_a, gate_x, bias_a, bias_x, soft)


def join_kernel(core_ref, *refs):
    out_ref = refs[-1]
    half = len(refs) // 2
    for core in range(2):
        order = refs[:half] + refs[half:-1] if core == 0 else refs[half:-1] + refs[:half]

        @pl.when(core_ref[0] == core)
        def _(order=order):
            out_ref[...] = jnp.concatenate([ref[...] for ref in order], 1).astype(BF16)


def join_columns(core, own, theirs):
    count, width = own[0].shape
    parts = own + theirs
    return pl.pallas_call(
        join_kernel,
        in_specs=[pl.BlockSpec(memory_space=pltpu.SMEM)] + [pl.BlockSpec(memory_space=pltpu.VMEM)] * len(parts),
        out_specs=pl.BlockSpec(memory_space=pltpu.VMEM),
        out_shape=jax.ShapeDtypeStruct((count, width * len(parts)), BF16),
        cost_estimate=pl.CostEstimate(
            flops=count * width * len(parts), bytes_accessed=6 * count * width * len(parts), transcendentals=0
        ),
    )(core, *parts)


def line_sum(value, axis):
    size = lax.axis_size(axis)
    if size == 1:
        return value
    if size % 2:
        return lax.psum(value, axis)
    me = lax.axis_index(axis)
    half = size // 2
    for hop in range(half - 1):
        value = value + lax.ppermute(value, axis, [(hop, hop + 1), (size - 1 - hop, size - 2 - hop)])
    value = value + lax.ppermute(value, axis, [(half - 1, half), (half, half - 1)])
    for hop in reversed(range(half - 1)):
        came = lax.ppermute(value, axis, [(hop + 1, hop), (size - 2 - hop, size - 1 - hop)])
        value = jnp.where((me == hop) | (me == size - 1 - hop), came, value)
    return value


def paired(inputs, out_grad, gate_a, gate_x, bias_a, bias_x, decay_param, segment_ids):
    count, chans = inputs.shape[1:]
    blocks, width = gate_a.shape[:2]
    per_core = blocks // 2
    half = chans // 2
    core = lax.axis_index("seq")
    first = core == 0
    swap = [(0, 1), (1, 0)]
    padded = (width // LANES + 1) * LANES

    def halves(value):
        low, high = value[:, :half], value[:, half:]
        return jnp.where(first, low, high), jnp.where(first, high, low)

    own_x, out_x = halves(inputs[0])
    own_dy, out_dy = halves(out_grad[0])
    seg = jnp.broadcast_to(segment_ids[0].astype(F32)[:, None], (count, LANES))
    core_arr = core.astype(jnp.int32).reshape(1)
    bias_a3, bias_x3 = bias_a.reshape(blocks, 1, width), bias_x.reshape(blocks, 1, width)
    soft3 = jax.nn.softplus(decay_param).reshape(blocks, 1, width)

    def cols(value, which):
        return value[:, which * width : (which + 1) * width]

    def widen(value):
        return jnp.pad(value.astype(F32), ((0, 0), (0, padded - value.shape[1])))

    others = []
    for which in range(per_core):
        sent = jnp.stack([widen(cols(out_x, which)), widen(cols(out_dy, which)), widen(seg)])
        others.append(lax.ppermute(sent, "seq", swap))
    own_ig, their_ig, totals = [], [], []
    for which in range(per_core):
        ga, gx, mine, theirs = run_block(
            which, core_arr, cols(own_x, which), cols(own_dy, which), others[which], seg,
            gate_a, gate_x, bias_a3, bias_x3, soft3,
        )
        own_ig.append(mine)
        their_ig.append(lax.ppermute(theirs, "seq", swap))
        totals.append([line_sum(ga, "dp"), line_sum(gx, "dp")])
    fetched = [[lax.ppermute(part, "seq", swap) for part in pair] for pair in totals]

    def ordered(mine, theirs, join):
        return jnp.where(first, join(mine + theirs), join(theirs + mine))

    input_grad = join_columns(core_arr, own_ig, their_ig)[None]
    whole_a = ordered([t[0] for t in totals], [t[0] for t in fetched], jnp.stack)
    whole_x = ordered([t[1] for t in totals], [t[1] for t in fetched], jnp.stack)
    return (
        input_grad,
        whole_a[:, :width],
        whole_x[:, :width],
        whole_a[:, width].reshape(chans),
        whole_x[:, width].reshape(chans),
        jax.nn.sigmoid(decay_param) * whole_a[:, width + 1].reshape(chans),
    )


def shards(inputs, out_grad, gate_a, gate_x, bias_a, bias_x, decay_param, segment_ids):
    batch, count, _ = inputs.shape
    if lax.axis_size("seq") == 2 and batch == 1 and gate_a.shape[0] % 2 == 0 and count % 128 == 0:
        body = paired
    else:
        body = general
    return body(inputs, out_grad, gate_a, gate_x, bias_a, bias_x, decay_param, segment_ids)


def solution(mesh):
    in_specs = (
        P("dp", "seq", "width"),
        P("dp", "seq", "width"),
        P("width", None, None),
        P("width", None, None),
        P("width"),
        P("width"),
        P("width"),
        P("dp", "seq"),
    )
    out_specs = (
        P("dp", "seq", "width"),
        P("width", None, None),
        P("width", None, None),
        P("width"),
        P("width"),
        P("width"),
    )
    return jax.shard_map(shards, mesh=mesh, in_specs=in_specs, out_specs=out_specs, check_vma=False)
```
